32 devices in a mesh: alpha: 2 (over x), beta: 16 (over z, y, core).
Axes of the slice: x: 2, y: 2, z: 4, core: 2. Of those that a mesh axis runs over, the one named last changes fastest.
Arguments:
- coef: bfloat16 [2048, 2048], P('alpha', 'beta'), may hold values from -6 to 6
- beta_ops: bfloat16 [2048, 512], P('beta'), may hold values from -0.25 to 0.25
- beta_cols: int32 [16, 4], P('beta'), may hold values from 0 to 15, as said below
- alpha_ops: bfloat16 [2048, 4096], P('alpha'), may hold values from -0.09375 to 0.09375
- alpha_cols: int32 [2, 4], P('alpha'), may hold values from 0 to 1, as said below
- pair_alpha: bfloat16 [2048, 576], P('alpha'), may hold values from -12 to 12
- pair_beta: bfloat16 [2048, 576], P('beta'), may hold values from -0.125 to 0.125
- pair_coupling: bfloat16 [576, 576], replicated, may hold values from -0.25 to 0.25
- denominators: float32 [2048, 2048], P('alpha', 'beta'), may hold values from 0.5 to 4
Outputs:
- sigma_scaled: float32 [2048, 2048], P('alpha', 'beta')
The draws below stay inside these ranges and needn't reach their ends.
Inputs may be any that keep to these rules, and one draw needn't show every extreme that they name: `beta_cols`: the 4 entries of row j are different and each lies within two blocks of j, counted around the beta blocks cyclically. `alpha_cols`: each entry of row i is i or one of its two neighbours, counted around the alpha blocks cyclically; entries may repeat.
All inputs are finite; a program needn't handle non-finite values.
Results may differ from the reference program's by a relative error of at most 0.013.
Values may be sent and summed in bfloat16 or wider, within the bound.
A program may use at most 128 MiB of HBM per device.

```python
import math
import jax
import jax.numpy as jnp
from jax import lax

RA = 1024
RB = 128
KB = 4
KA = 4
P_SIZE = 576
NA = 2048
NB = 2048
N_ALPHA = 2
N_BETA = 16


def draw_beta_cols(key, part):
    keys = jax.random.split(jax.random.fold_in(key, 11), N_BETA)
    offsets = jax.vmap(lambda single: jax.random.permutation(single, 5)[:KB])(keys) - 2
    rows = jnp.arange(N_BETA, dtype=jnp.int32)[:, None]
    return ((rows + offsets + N_BETA) % N_BETA).astype(jnp.int32)


def draw_alpha_cols(key, part):
    base = jax.random.fold_in(key, 23)
    free_offsets = jax.random.randint(jax.random.fold_in(base, 1), (N_ALPHA, KA - 2), -1, 2)
    fixed_offsets = jnp.broadcast_to(jnp.array([-1, 1], dtype=jnp.int32)[None, :], (N_ALPHA, 2))
    offsets = jnp.concatenate([fixed_offsets, free_offsets.astype(jnp.int32)], axis=1)
    keys = jax.random.split(jax.random.fold_in(base, 2), N_ALPHA)
    orders = jax.vmap(lambda single: jax.random.permutation(single, KA))(keys)
    offsets = jnp.take_along_axis(offsets, orders.astype(jnp.int32), axis=1)
    rows = jnp.arange(N_ALPHA, dtype=jnp.int32)[:, None]
    return ((rows + offsets + N_ALPHA) % N_ALPHA).astype(jnp.int32)


def block_scale(stream_key, extent, shards, least, top_value):
    loudness, own = 1.0, jax.random.fold_in(stream_key, 6)
    for position, shards_of in shards:
        steps = jnp.exp(jax.random.uniform(jax.random.fold_in(own, position), (shards_of,), jnp.float32, least / len(shards), top_value / len(shards)))
        loudness = loudness * jnp.repeat(steps, extent[position] // shards_of).reshape([-1 if axis == position else 1 for axis in range(len(extent))])
    return loudness


def scatter_about(stream_key, dims, width, limit, shards=(), kind=jnp.bfloat16):
    values = jax.random.normal(stream_key, dims, jnp.float32) * width
    if len(shards) > 0:
        values = block_scale(stream_key, dims, shards, -0.22, 0.18) * values
    return jnp.clip(values, min=-limit, max=limit).astype(kind)


def setup_inputs(seed: int = 0) -> dict:
    key_list = jax.random.split(jax.random.key(seed), 10)
    coef = scatter_about(key_list[0], (NA, NB), 1.0, 6.0, ((0, 2), (1, 16)))
    beta_ops = scatter_about(key_list[1], (NB, KB * RB), (KB * RB) ** -0.5, 0.25, ((0, 16),))
    beta_cols = draw_beta_cols(jax.random.fold_in(key_list[9], 71), 0)
    alpha_ops = scatter_about(key_list[3], (NA, KA * RA), (KA * RA) ** -0.5, 0.09375, ((0, 2),))
    alpha_cols = draw_alpha_cols(jax.random.fold_in(key_list[9], 71), 0)
    pair_alpha = scatter_about(key_list[5], (NA, P_SIZE), 2.0, 12.0, ((0, 2),))
    pair_beta = scatter_about(key_list[6], (NB, P_SIZE), NB ** -0.5, 0.125, ((0, 16),))
    pair_coupling = scatter_about(key_list[7], (P_SIZE, P_SIZE), P_SIZE ** -0.5, 0.25)
    denominators = jnp.clip(jnp.exp(math.log(4.0) - 2.0794415 * jax.random.uniform(key_list[8], (NA, NB), jnp.float32) ** block_scale(key_list[8], (NA, NB), ((0, 2), (1, 16)), -0.2, 0.2)), 0.5, 4.0)
    return {"coef": coef, "beta_ops": beta_ops, "beta_cols": beta_cols, "alpha_ops": alpha_ops, "alpha_cols": alpha_cols, "pair_alpha": pair_alpha, "pair_beta": pair_beta, "pair_coupling": pair_coupling, "denominators": denominators}


def reference(coef, beta_ops, beta_cols, alpha_ops, alpha_cols, pair_alpha, pair_beta, pair_coupling, denominators):
    def beta_block(index):
        blocks = lax.dynamic_slice_in_dim(beta_ops, index * RB, RB, 0)
        total = jnp.zeros((coef.shape[0], RB), jnp.float32)
        for listed in range(KB):
            source = lax.dynamic_slice_in_dim(coef, (beta_cols[index, listed] * RB).astype(jnp.int32), RB, 1)
            tile_part = blocks[:, listed * RB:(listed + 1) * RB]
            total = total + lax.dot_general(source, tile_part, (((1,), (1,)), ((), ())), preferred_element_type=jnp.float32)
        return total

    same_beta = lax.map(beta_block, jnp.arange(N_BETA, dtype=jnp.int32))
    same_beta = jnp.transpose(same_beta, (1, 0, 2)).reshape(coef.shape[0], coef.shape[1])

    def alpha_block(index):
        blocks = lax.dynamic_slice_in_dim(alpha_ops, index * RA, RA, 0)
        total = jnp.zeros((RA, coef.shape[1]), jnp.float32)
        for listed in range(KA):
            source = lax.dynamic_slice_in_dim(coef, (alpha_cols[index, listed] * RA).astype(jnp.int32), RA, 0)
            tile_part = blocks[:, listed * RA:(listed + 1) * RA]
            total = total + jnp.dot(tile_part, source, preferred_element_type=jnp.float32)
        return total

    same_alpha = lax.map(alpha_block, jnp.arange(N_ALPHA, dtype=jnp.int32))
    same_alpha = same_alpha.reshape(coef.shape[0], coef.shape[1])

    density = jnp.dot(coef, pair_beta, preferred_element_type=jnp.float32).astype(jnp.bfloat16)
    excited = (jnp.dot(density, pair_coupling, preferred_element_type=jnp.float32) * pair_alpha.astype(jnp.float32)).astype(jnp.bfloat16)
    mixed = lax.dot_general(excited, pair_beta, (((1,), (1,)), ((), ())), preferred_element_type=jnp.float32)
    return (same_beta + same_alpha + mixed) / denominators
```

```python
import functools

import jax
import jax.numpy as jnp
from jax import lax
from jax.experimental import pallas as pl
from jax.experimental.pallas import tpu as pltpu
from jax.sharding import PartitionSpec as P

MESH = pl.DeviceIdType.MESH
GROUP = 4
REACH = 2
F32 = jnp.float32
BF16 = jnp.bfloat16


def kernel(
    n_alpha,
    n_beta,
    beta_cols,
    alpha_cols,
    coef_in,
    ops_in,
    alpha_in,
    pair_alpha_in,
    pair_beta_in,
    coupling_in,
    out,
    coef,
    ops,
    alpha_ops,
    pair_alpha,
    pair_beta,
    coupling,
    near,
    window,
    part,
    part_in,
    excited,
    both,
    back,
    back_in,
    local_sem,
    alpha_sem,
    coef_send,
    coef_recv,
    pair_send,
    pair_recv,
    near_send,
    near_recv,
    back_send,
    back_recv,
    part_send,
    part_recv,
    exc_send,
    exc_recv,
    halo_send,
    halo_recv,
    nbr_send,
    nbr_recv,
):
    a = lax.axis_index("alpha")
    b = lax.axis_index("beta")
    outer = n_beta // GROUP
    g = b % GROUP
    z = b // GROUP
    rows, width = coef.shape[1], coef.shape[2]
    strip = rows // GROUP
    share = strip // outer
    listed = beta_cols.shape[1]
    alpha_listed = alpha_cols.shape[1]
    pairs = coupling.shape[0]

    def local(index, src, dst, sem=None):
        copy = pltpu.make_async_copy(src, dst, local_sem.at[index] if sem is None else sem)
        copy.start()
        return copy

    def remote(src, dst, send, recv, target):
        copy = pltpu.make_async_remote_copy(
            src_ref=src,
            dst_ref=dst,
            send_sem=send,
            recv_sem=recv,
            device_id=target,
            device_id_type=MESH,
        )
        copy.start()
        return copy

    def mate(d):
        return (a, z * GROUP + (g + d) % GROUP)

    def plane(d):
        return (a, ((z + d) % outer) * GROUP + g)

    alpha_steps = [1] if n_alpha > 1 else []
    if n_alpha > 2:
        alpha_steps.append(n_alpha - 1)

    own_coef = local(0, coef_in, coef.at[0])
    own_pair = local(1, pair_beta_in, pair_beta.at[g])
    own_strip = local(
        2, coef_in.at[pl.ds(pl.multiple_of(g * strip, strip), strip)], window.at[REACH + g]
    )
    own_ops = local(3, ops_in, ops)
    own_coupling = local(4, coupling_in, coupling)
    first = pl.multiple_of(g * strip + z * share, share)
    own_rows = local(5, pair_alpha_in.at[pl.ds(first, share)], pair_alpha)
    alpha_copy = local(0, alpha_in, alpha_ops, alpha_sem)

    barrier = pltpu.get_barrier_semaphore()
    partners = 0
    for d in range(1, GROUP):
        pl.semaphore_signal(barrier, inc=1, device_id=mate(d), device_id_type=MESH)
        partners += 1
    for d in range(1, outer):
        pl.semaphore_signal(barrier, inc=1, device_id=plane(d), device_id_type=MESH)
        partners += 1
    for d in alpha_steps:
        pl.semaphore_signal(
            barrier, inc=1, device_id=((a + d) % n_alpha, b), device_id_type=MESH
        )
        partners += 1
    pl.semaphore_wait(barrier, partners)

    own_coef.wait()
    coef_copies = []
    for d in (2, 3, 1):
        h = (g + d) % GROUP
        coef_copies.append(
            remote(
                coef.at[0, pl.ds(pl.multiple_of(h * strip, strip), strip)],
                window.at[REACH + g],
                coef_send.at[d],
                coef_recv.at[d],
                mate(d),
            )
        )
    own_pair.wait()
    pair_copies = [
        remote(
            pair_beta.at[g], pair_beta.at[g], pair_send.at[d], pair_recv.at[d], mate(d)
        )
        for d in (2, 3, 1)
    ]
    alpha_copies = [
        remote(
            coef.at[0],
            coef.at[2 - i if n_alpha > 2 else 1],
            nbr_send.at[i],
            nbr_recv.at[i],
            ((a + d) % n_alpha, b),
        )
        for i, d in enumerate(alpha_steps)
    ]

    own_ops.wait()
    tiles = [ops[:, k * width : (k + 1) * width] for k in range(listed)]
    slots = [(beta_cols[0, k] - b + REACH + n_beta) % n_beta for k in range(listed)]
    for s in range(2 * REACH + 1):
        total = jnp.zeros(tiles[0].shape, F32)
        for k in range(listed):
            chosen = (slots[k] == s).astype(F32)
            total = total + tiles[k].astype(F32) * chosen
        near[g, :, s * width : (s + 1) * width] = total.astype(BF16)
    near_copies = [
        remote(near.at[g], near.at[g], near_send.at[d], near_recv.at[d], mate(d))
        for d in (2, 3, 1)
    ]

    own_strip.wait()
    for copy in coef_copies:
        copy.wait_recv()
    halo_copies = [
        remote(
            window.at[pl.ds(GROUP, REACH)],
            window.at[pl.ds(0, REACH)],
            halo_send.at[0],
            halo_recv.at[0],
            plane(1),
        ),
        remote(
            window.at[pl.ds(REACH, REACH)],
            window.at[pl.ds(REACH + GROUP, REACH)],
            halo_send.at[1],
            halo_recv.at[1],
            plane(outer - 1),
        ),
    ]
    for copy in pair_copies:
        copy.wait_recv()

    strips = jnp.concatenate([window[REACH + i] for i in range(GROUP)], axis=1)
    plane_pairs = pair_beta[...].reshape(GROUP * width, pairs)
    density = jnp.dot(strips, plane_pairs, preferred_element_type=F32)
    part[...] = density.astype(BF16).reshape(outer, share, pairs)
    part_copies = [
        remote(
            part.at[(z + d) % outer],
            part_in.at[d - 1],
            part_send.at[d - 1],
            part_recv.at[d - 1],
            plane(d),
        )
        for d in range(1, outer)
    ]

    for copy in alpha_copies:
        copy.wait_recv()
    alpha_copy.wait()
    blocks = []
    for k in range(alpha_listed):
        off = (alpha_cols[0, k] - a + n_alpha) % n_alpha
        blocks.append(jnp.minimum(off, 1) + jnp.where(off > 1, 1, 0) if n_alpha > 2 else off)

    def alpha_step(i, carry):
        at = pl.ds(pl.multiple_of(i * strip, strip), strip)
        total = jnp.zeros((strip, width), F32)
        for k in range(alpha_listed):
            total = total + jnp.dot(
                alpha_ops[at, k * rows : (k + 1) * rows],
                coef[blocks[k]],
                preferred_element_type=F32,
            )
        out[at, :] = total
        return carry

    lax.fori_loop(0, GROUP, alpha_step, 0)

    for copy in part_copies:
        copy.wait_recv()
    total = part[z].astype(F32)
    for d in range(1, outer):
        total = total + part_in[d - 1].astype(F32)
    own_coupling.wait()
    own_rows.wait()
    raised = jnp.dot(total.astype(BF16), coupling[...], preferred_element_type=F32)
    excited[z] = (raised * pair_alpha[...].astype(F32)).astype(BF16)
    exc_copies = [
        remote(
            excited.at[z], excited.at[z], exc_send.at[d - 1], exc_recv.at[d - 1], plane(d)
        )
        for d in range(1, outer)
    ]

    for copy in near_copies:
        copy.wait_recv()
    for copy in halo_copies:
        copy.wait_recv()
    for i in range(GROUP):
        around = jnp.concatenate([window[i + s] for s in range(2 * REACH + 1)], axis=1)
        both[i] = lax.dot_general(
            around, near[i], (((1,), (1,)), ((), ())), preferred_element_type=F32
        )

    for copy in exc_copies:
        copy.wait_recv()
    rows_excited = excited[...].reshape(strip, pairs)
    back_copies = []
    for d in (2, 3, 1, 0):
        h = (g + d) % GROUP
        mixed = lax.dot_general(
            rows_excited, pair_beta[h], (((1,), (1,)), ((), ())), preferred_element_type=F32
        )
        if d == 0:
            at = pl.ds(pl.multiple_of(g * strip, strip), strip)
            out[at, :] = out[at, :] + (mixed + both[h])
        else:
            back[d - 1] = (mixed + both[h]).astype(BF16)
            back_copies.append(
                (
                    d,
                    remote(
                        back.at[d - 1],
                        back_in.at[d - 1],
                        back_send.at[d - 1],
                        back_recv.at[d - 1],
                        mate(d),
                    ),
                )
            )
    for d, copy in sorted(back_copies, key=lambda pair: pair[0]):
        copy.wait_recv()
        h = (g + GROUP - d) % GROUP
        at = pl.ds(pl.multiple_of(h * strip, strip), strip)
        out[at, :] = out[at, :] + back_in[d - 1].astype(F32)

    everything = coef_copies + pair_copies + alpha_copies + near_copies + halo_copies
    everything += part_copies + exc_copies + [copy for _, copy in back_copies]
    for copy in everything:
        copy.wait_send()


def local(
    coef,
    beta_ops,
    beta_cols,
    alpha_ops,
    alpha_cols,
    pair_alpha,
    pair_beta,
    pair_coupling,
    denominators,
):
    n_alpha = lax.axis_size("alpha")
    n_beta = lax.axis_size("beta")
    rows, width = coef.shape
    pairs = pair_beta.shape[1]
    outer = n_beta // GROUP
    strip = rows // GROUP
    share = strip // outer
    span = 2 * REACH + 1
    dma = pltpu.SemaphoreType.DMA
    vmem, smem, anywhere = (
        pl.BlockSpec(memory_space=pltpu.VMEM),
        pl.BlockSpec(memory_space=pltpu.SMEM),
        pl.BlockSpec(memory_space=pl.ANY),
    )
    summed = pl.pallas_call(
        functools.partial(kernel, n_alpha, n_beta),
        out_shape=jax.ShapeDtypeStruct((rows, width), F32),
        in_specs=[smem, smem] + [anywhere] * 6,
        out_specs=vmem,
        scratch_shapes=[
            pltpu.VMEM((min(n_alpha, 3), rows, width), BF16),
            pltpu.VMEM(beta_ops.shape, BF16),
            pltpu.VMEM(alpha_ops.shape, BF16),
            pltpu.VMEM((share, pairs), BF16),
            pltpu.VMEM((GROUP, width, pairs), BF16),
            pltpu.VMEM((pairs, pairs), BF16),
            pltpu.VMEM((GROUP, width, span * width), BF16),
            pltpu.VMEM((GROUP + 2 * REACH, strip, width), BF16),
            pltpu.VMEM((outer, share, pairs), BF16),
            pltpu.VMEM((outer - 1, share, pairs), BF16),
            pltpu.VMEM((outer, share, pairs), BF16),
            pltpu.VMEM((GROUP, strip, width), F32),
            pltpu.VMEM((GROUP - 1, strip, width), BF16),
            pltpu.VMEM((GROUP - 1, strip, width), BF16),
            dma((6,)),
            dma,
            dma((GROUP,)),
            dma((GROUP,)),
            dma((GROUP,)),
            dma((GROUP,)),
            dma((GROUP,)),
            dma((GROUP,)),
            dma((GROUP - 1,)),
            dma((GROUP - 1,)),
            dma((outer - 1,)),
            dma((outer - 1,)),
            dma((outer - 1,)),
            dma((outer - 1,)),
            dma((2,)),
            dma((2,)),
            dma((2,)),
            dma((2,)),
        ],
        compiler_params=pltpu.CompilerParams(collective_id=0, has_side_effects=True),
    )(beta_cols, alpha_cols, coef, beta_ops, alpha_ops, pair_alpha, pair_beta, pair_coupling)
    return summed / denominators


def solution(mesh):
    return jax.shard_map(
        local,
        mesh=mesh,
        in_specs=(
            P("alpha", "beta"),
            P("beta", None),
            P("beta", None),
            P("alpha", None),
            P("alpha", None),
            P("alpha", None),
            P("beta", None),
            P(),
            P("alpha", "beta"),
        ),
        out_specs=P("alpha", "beta"),
        check_vma=False,
    )
```

```python
import functools

import jax
import jax.numpy as jnp
from jax import lax
from jax.experimental import pallas as pl
from jax.experimental.pallas import tpu as pltpu
from jax.sharding import PartitionSpec as P

MESH = pl.DeviceIdType.MESH
GROUP = 4
REACH = 2
F32 = jnp.float32
BF16 = jnp.bfloat16


def kernel(
    n_alpha,
    n_beta,
    beta_cols,
    alpha_cols,
    coef_in,
    ops_in,
    alpha_in,
    pair_alpha_in,
    pair_beta_in,
    coupling_in,
    out,
    coef,
    ops,
    alpha_ops,
    pair_tile,
    pair_alpha,
    pair_beta,
    coupling,
    near,
    window,
    part,
    part_in,
    excited,
    both,
    back,
    back_in,
    local_sem,
    alpha_sem,
    coef_send,
    coef_recv,
    pair_send,
    pair_recv,
    near_send,
    near_recv,
    back_send,
    back_recv,
    part_send,
    part_recv,
    exc_send,
    exc_recv,
    halo_send,
    halo_recv,
    nbr_send,
    nbr_recv,
):
    a = lax.axis_index("alpha")
    b = lax.axis_index("beta")
    outer = n_beta // GROUP
    g = b % GROUP
    z = b // GROUP
    rows, width = coef.shape[1], coef.shape[2]
    strip = rows // GROUP
    share = strip // outer
    listed = beta_cols.shape[1]
    alpha_listed = alpha_cols.shape[1]
    pairs = coupling.shape[0]

    def local(index, src, dst, sem=None):
        copy = pltpu.make_async_copy(src, dst, local_sem.at[index] if sem is None else sem)
        copy.start()
        return copy

    def remote(src, dst, send, recv, target):
        copy = pltpu.make_async_remote_copy(
            src_ref=src,
            dst_ref=dst,
            send_sem=send,
            recv_sem=recv,
            device_id=target,
            device_id_type=MESH,
        )
        copy.start()
        return copy

    def mate(d):
        return (a, z * GROUP + (g + d) % GROUP)

    core_mate = (a, z * GROUP + (g // 2) * 2 + 1 - g % 2)
    across = (1 - g // 2) * 2 + g % 2
    chip_mate = (a, z * GROUP + across)

    def plane(d):
        return (a, ((z + d) % outer) * GROUP + g)

    alpha_steps = [1] if n_alpha > 1 else []
    if n_alpha > 2:
        alpha_steps.append(n_alpha - 1)

    own_coef = local(0, coef_in, coef.at[0])
    own_pair = local(1, pair_beta_in, pair_beta.at[g])
    own_strip = local(
        2, coef_in.at[pl.ds(pl.multiple_of(g * strip, strip), strip)], window.at[REACH + g]
    )
    own_ops = local(3, ops_in, ops)
    own_coupling = local(4, coupling_in, coupling)
    first = pl.multiple_of(g * strip + z * share, share)
    lanes = pair_tile.shape[1]
    own_rows = local(
        5, pair_alpha_in.at[:, pl.ds(pl.multiple_of(first // lanes * lanes, lanes), lanes)], pair_tile
    )
    alpha_copy = local(0, alpha_in, alpha_ops, alpha_sem)

    barrier = pltpu.get_barrier_semaphore()
    partners = 0
    for d in range(1, GROUP):
        pl.semaphore_signal(barrier, inc=1, device_id=mate(d), device_id_type=MESH)
        partners += 1
    for d in range(1, outer):
        pl.semaphore_signal(barrier, inc=1, device_id=plane(d), device_id_type=MESH)
        partners += 1
    for d in alpha_steps:
        pl.semaphore_signal(
            barrier, inc=1, device_id=((a + d) % n_alpha, b), device_id_type=MESH
        )
        partners += 1
    pl.semaphore_wait(barrier, partners)

    own_coef.wait()
    coef_copies = []
    for d in (2, 3, 1):
        h = (g + d) % GROUP
        coef_copies.append(
            remote(
                coef.at[0, pl.ds(pl.multiple_of(h * strip, strip), strip)],
                window.at[REACH + g],
                coef_send.at[d],
                coef_recv.at[d],
                mate(d),
            )
        )
    own_pair.wait()
    pair_copies = [
        remote(pair_beta.at[g], pair_beta.at[g], pair_send.at[i], pair_recv.at[i], target)
        for i, target in enumerate((chip_mate, core_mate))
    ]
    alpha_copies = [
        remote(
            coef.at[0],
            coef.at[2 - i if n_alpha > 2 else 1],
            nbr_send.at[i],
            nbr_recv.at[i],
            ((a + d) % n_alpha, b),
        )
        for i, d in enumerate(alpha_steps)
    ]

    own_ops.wait()
    tiles = [ops[:, k * width : (k + 1) * width] for k in range(listed)]
    slots = [(beta_cols[0, k] - b + REACH + n_beta) % n_beta for k in range(listed)]
    for s in range(2 * REACH + 1):
        total = jnp.zeros(tiles[0].shape, F32)
        for k in range(listed):
            chosen = (slots[k] == s).astype(F32)
            total = total + tiles[k].astype(F32) * chosen
        near[g, :, s * width : (s + 1) * width] = total.astype(BF16)
    near_copies = [
        remote(near.at[g], near.at[g], near_send.at[i], near_recv.at[i], target)
        for i, target in enumerate((chip_mate, core_mate))
    ]

    own_strip.wait()
    for copy in coef_copies:
        copy.wait_recv()
    halo_copies = [
        remote(
            window.at[pl.ds(GROUP, REACH)],
            window.at[pl.ds(0, REACH)],
            halo_send.at[0],
            halo_recv.at[0],
            plane(1),
        ),
        remote(
            window.at[pl.ds(REACH, REACH)],
            window.at[pl.ds(REACH + GROUP, REACH)],
            halo_send.at[1],
            halo_recv.at[1],
            plane(outer - 1),
        ),
    ]
    pair_copies[0].wait_recv()
    pair_copies.append(
        remote(
            pair_beta.at[across],
            pair_beta.at[across],
            pair_send.at[2],
            pair_recv.at[2],
            core_mate,
        )
    )
    for copy in pair_copies[1:]:
        copy.wait_recv()

    strips = jnp.concatenate([window[REACH + i] for i in range(GROUP)], axis=1)
    plane_pairs = jnp.concatenate([pair_beta[i] for i in range(GROUP)], axis=1)
    density = lax.dot_general(
        strips, plane_pairs, (((1,), (1,)), ((), ())), preferred_element_type=F32
    )
    part[...] = density.astype(BF16).reshape(outer, share, pairs)
    part_copies = [
        remote(
            part.at[(z + d) % outer],
            part_in.at[d - 1],
            part_send.at[d - 1],
            part_recv.at[d - 1],
            plane(d),
        )
        for d in range(1, outer)
    ]

    for copy in alpha_copies:
        copy.wait_recv()
    alpha_copy.wait()
    blocks = []
    for k in range(alpha_listed):
        off = (alpha_cols[0, k] - a + n_alpha) % n_alpha
        blocks.append(jnp.minimum(off, 1) + jnp.where(off > 1, 1, 0) if n_alpha > 2 else off)

    def alpha_step(i, carry):
        at = pl.ds(pl.multiple_of(i * strip, strip), strip)
        total = jnp.zeros((strip, width), F32)
        for k in range(alpha_listed):
            total = total + jnp.dot(
                alpha_ops[at, k * rows : (k + 1) * rows],
                coef[blocks[k]],
                preferred_element_type=F32,
            )
        out[at, :] = total
        return carry

    lax.fori_loop(0, GROUP, alpha_step, 0)

    near_copies[0].wait_recv()
    near_copies.append(
        remote(
            near.at[across], near.at[across], near_send.at[2], near_recv.at[2], core_mate
        )
    )
    own_rows.wait()
    pair_alpha[...] = jnp.transpose(pair_tile[...].astype(F32))
    own_coupling.wait()

    for copy in part_copies:
        copy.wait_recv()
    total = part[z].astype(F32)
    for d in range(1, outer):
        total = total + part_in[d - 1].astype(F32)
    raised = jnp.dot(total.astype(BF16), coupling[...], preferred_element_type=F32)
    excited[z] = (raised * pair_alpha[pl.ds(pl.multiple_of(first % lanes, share), share), :]).astype(
        BF16
    )
    exc_copies = [
        remote(
            excited.at[z], excited.at[z], exc_send.at[d - 1], exc_recv.at[d - 1], plane(d)
        )
        for d in range(1, outer)
    ]

    for copy in near_copies[1:]:
        copy.wait_recv()
    for copy in halo_copies:
        copy.wait_recv()
    for i in range(GROUP):
        around = jnp.concatenate([window[i + s] for s in range(2 * REACH + 1)], axis=1)
        both[:, i * width : (i + 1) * width] = lax.dot_general(
            around, near[i], (((1,), (1,)), ((), ())), preferred_element_type=F32
        )

    back_copies = []
    for e in range(outer):
        if e > 0:
            exc_copies[e - 1].wait_recv()
        y = (z + outer - e) % outer
        mixed = jnp.dot(excited[y], plane_pairs, preferred_element_type=F32)
        mixed = mixed + both[pl.ds(pl.multiple_of(y * share, share), share), :]
        for i in range(GROUP):
            back[i, y] = mixed[:, i * width : (i + 1) * width].astype(BF16)
        for d in range(1, GROUP):
            back_copies.append(
                (
                    d,
                    y,
                    remote(
                        back.at[(g + d) % GROUP, y],
                        back_in.at[d - 1, y],
                        back_send.at[e, d],
                        back_recv.at[e, d],
                        mate(d),
                    ),
                )
            )
        at = pl.ds(pl.multiple_of(g * strip + y * share, share), share)
        out[at, :] = out[at, :] + back[g, y].astype(F32)
    for d, y, copy in back_copies:
        copy.wait_recv()
        h = (g + GROUP - d) % GROUP
        at = pl.ds(pl.multiple_of(h * strip + y * share, share), share)
        out[at, :] = out[at, :] + back_in[d - 1, y].astype(F32)

    everything = coef_copies + pair_copies + alpha_copies + near_copies + halo_copies
    everything += part_copies + exc_copies + [copy for _, _, copy in back_copies]
    for copy in everything:
        copy.wait_send()


def local(
    coef,
    beta_ops,
    beta_cols,
    alpha_ops,
    alpha_cols,
    pair_alpha,
    pair_beta,
    pair_coupling,
    denominators,
):
    n_alpha = lax.axis_size("alpha")
    n_beta = lax.axis_size("beta")
    rows, width = coef.shape
    pairs = pair_beta.shape[1]
    outer = n_beta // GROUP
    strip = rows // GROUP
    share = strip // outer
    lanes = max(width, share)
    span = 2 * REACH + 1
    dma = pltpu.SemaphoreType.DMA
    vmem, smem, anywhere = (
        pl.BlockSpec(memory_space=pltpu.VMEM),
        pl.BlockSpec(memory_space=pltpu.SMEM),
        pl.BlockSpec(memory_space=pl.ANY),
    )
    summed = pl.pallas_call(
        functools.partial(kernel, n_alpha, n_beta),
        out_shape=pltpu.VMEM((rows, width), F32),
        in_specs=[smem, smem] + [anywhere] * 6,
        out_specs=vmem,
        scratch_shapes=[
            pltpu.VMEM((min(n_alpha, 3), rows, width), BF16),
            pltpu.VMEM(beta_ops.shape, BF16),
            pltpu.VMEM(alpha_ops.shape, BF16),
            pltpu.VMEM((pairs, lanes), BF16),
            pltpu.VMEM((lanes, pairs), F32),
            pltpu.VMEM((GROUP, pairs, width), BF16),
            pltpu.VMEM((pairs, pairs), BF16),
            pltpu.VMEM((GROUP, width, span * width), BF16),
            pltpu.VMEM((GROUP + 2 * REACH, strip, width), BF16),
            pltpu.VMEM((outer, share, pairs), BF16),
            pltpu.VMEM((outer - 1, share, pairs), BF16),
            pltpu.VMEM((outer, share, pairs), BF16),
            pltpu.VMEM((strip, GROUP * width), F32),
            pltpu.VMEM((GROUP, outer, share, width), BF16),
            pltpu.VMEM((GROUP - 1, outer, share, width), BF16),
            dma((6,)),
            dma,
            dma((GROUP,)),
            dma((GROUP,)),
            dma((GROUP,)),
            dma((GROUP,)),
            dma((GROUP,)),
            dma((GROUP,)),
            dma((outer, GROUP)),
            dma((outer, GROUP)),
            dma((outer - 1,)),
            dma((outer - 1,)),
            dma((outer - 1,)),
            dma((outer - 1,)),
            dma((2,)),
            dma((2,)),
            dma((2,)),
            dma((2,)),
        ],
        compiler_params=pltpu.CompilerParams(collective_id=0, has_side_effects=True),
    )(beta_cols, alpha_cols, coef, beta_ops, alpha_ops, pair_alpha.T, pair_beta.T, pair_coupling)
    return summed / denominators


def solution(mesh):
    return jax.shard_map(
        local,
        mesh=mesh,
        in_specs=(
            P("alpha", "beta"),
            P("beta", None),
            P("beta", None),
            P("alpha", None),
            P("alpha", None),
            P("alpha", None),
            P("beta", None),
            P(),
            P("alpha", "beta"),
        ),
        out_specs=P("alpha", "beta"),
        check_vma=False,
    )
```

```python
import functools

import jax
import jax.numpy as jnp
from jax import lax
from jax.experimental import pallas as pl
from jax.experimental.pallas import tpu as pltpu
from jax.sharding import PartitionSpec as P

MESH = pl.DeviceIdType.MESH
GROUP = 4
PIECES = 2
REACH = 2
F32 = jnp.float32
BF16 = jnp.bfloat16


def kernel(
    n_alpha,
    n_beta,
    beta_cols,
    alpha_cols,
    coef_in,
    ops_in,
    alpha_in,
    pair_alpha_in,
    pair_beta_in,
    coupling_in,
    out,
    coef,
    ops,
    alpha_ops,
    pair_tile,
    pair_alpha,
    pair_beta,
    coupling,
    near,
    window,
    part,
    part_in,
    excited,
    both,
    back,
    back_in,
    local_sem,
    alpha_sem,
    coef_send,
    coef_recv,
    pair_send,
    pair_recv,
    near_send,
    near_recv,
    back_send,
    back_recv,
    part_send,
    part_recv,
    exc_send,
    exc_recv,
    halo_send,
    halo_recv,
    nbr_send,
    nbr_recv,
):
    a = lax.axis_index("alpha")
    b = lax.axis_index("beta")
    outer = n_beta // GROUP
    g = b % GROUP
    z = b // GROUP
    rows, width = coef.shape[1], coef.shape[2]
    strip = rows // GROUP
    share = strip // outer
    sub = share // PIECES
    listed = beta_cols.shape[1]
    alpha_listed = alpha_cols.shape[1]
    pairs = coupling.shape[0]

    def local(index, src, dst, sem=None):
        copy = pltpu.make_async_copy(src, dst, local_sem.at[index] if sem is None else sem)
        copy.start()
        return copy

    def remote(src, dst, send, recv, target):
        copy = pltpu.make_async_remote_copy(
            src_ref=src,
            dst_ref=dst,
            send_sem=send,
            recv_sem=recv,
            device_id=target,
            device_id_type=MESH,
        )
        copy.start()
        return copy

    def mate(d):
        return (a, z * GROUP + (g + d) % GROUP)

    core_mate = (a, z * GROUP + (g // 2) * 2 + 1 - g % 2)
    across = (1 - g // 2) * 2 + g % 2
    chip_mate = (a, z * GROUP + across)

    def plane(d):
        return (a, ((z + d) % outer) * GROUP + g)

    far_first = sorted(range(1, outer), key=lambda d: -min(d, outer - d))
    alpha_steps = [1] if n_alpha > 1 else []
    if n_alpha > 2:
        alpha_steps.append(n_alpha - 1)

    own_coef = local(0, coef_in, coef.at[0])
    own_pair = local(1, pair_beta_in, pair_beta.at[g])
    own_strip = local(
        2, coef_in.at[pl.ds(pl.multiple_of(g * strip, strip), strip)], window.at[REACH + g]
    )
    own_ops = local(3, ops_in, ops)
    own_coupling = local(4, coupling_in, coupling)
    first = pl.multiple_of(g * strip + z * share, share)
    lanes = pair_tile.shape[1]
    own_rows = local(
        5, pair_alpha_in.at[:, pl.ds(pl.multiple_of(first // lanes * lanes, lanes), lanes)], pair_tile
    )
    alpha_copy = local(0, alpha_in, alpha_ops, alpha_sem)

    barrier = pltpu.get_barrier_semaphore()
    partners = 0
    for d in range(1, GROUP):
        pl.semaphore_signal(barrier, inc=1, device_id=mate(d), device_id_type=MESH)
        partners += 1
    for d in range(1, outer):
        pl.semaphore_signal(barrier, inc=1, device_id=plane(d), device_id_type=MESH)
        partners += 1
    for d in alpha_steps:
        pl.semaphore_signal(
            barrier, inc=1, device_id=((a + d) % n_alpha, b), device_id_type=MESH
        )
        partners += 1
    pl.semaphore_wait(barrier, partners)

    own_coef.wait()
    beside = (g // 2) * 2 + 1 - g % 2
    opposite = (1 - g // 2) * 2 + 1 - g % 2
    coef_copies = [
        remote(
            coef.at[0, pl.ds(pl.multiple_of(h * strip, strip), strip)],
            window.at[REACH + g],
            coef_send.at[i],
            coef_recv.at[i],
            (a, z * GROUP + h),
        )
        for i, h in enumerate((beside, across, opposite))
    ]
    own_pair.wait()
    pair_copies = [
        remote(pair_beta.at[g], pair_beta.at[g], pair_send.at[i], pair_recv.at[i], target)
        for i, target in enumerate((chip_mate, core_mate))
    ]
    alpha_copies = [
        remote(
            coef.at[0],
            coef.at[2 - i if n_alpha > 2 else 1],
            nbr_send.at[i],
            nbr_recv.at[i],
            ((a + d) % n_alpha, b),
        )
        for i, d in enumerate(alpha_steps)
    ]

    own_ops.wait()
    tiles = [ops[:, k * width : (k + 1) * width] for k in range(listed)]
    slots = [(beta_cols[0, k] - b + REACH + n_beta) % n_beta for k in range(listed)]
    for s in range(2 * REACH + 1):
        total = jnp.zeros(tiles[0].shape, F32)
        for k in range(listed):
            chosen = (slots[k] == s).astype(F32)
            total = total + tiles[k].astype(F32) * chosen
        near[g, :, s * width : (s + 1) * width] = total.astype(BF16)
    near_copies = [
        remote(near.at[g], near.at[g], near_send.at[i], near_recv.at[i], target)
        for i, target in enumerate((chip_mate, core_mate))
    ]

    half = g // 2
    own_strip.wait()
    coef_copies[0].wait_recv()
    halo_copies = []
    for side in (half, 1 - half):
        if len(halo_copies) == 1:
            coef_copies[1].wait_recv()
            coef_copies[2].wait_recv()
        halo_copies.append(
            remote(
                window.at[pl.ds(REACH + side * (GROUP - REACH), REACH)],
                window.at[pl.ds((1 - side) * (REACH + GROUP), REACH)],
                halo_send.at[side],
                halo_recv.at[side],
                plane(side + (1 - side) * (outer - 1)),
            )
        )
    pair_copies[0].wait_recv()
    pair_copies.append(
        remote(
            pair_beta.at[across],
            pair_beta.at[across],
            pair_send.at[2],
            pair_recv.at[2],
            core_mate,
        )
    )
    for copy in pair_copies[1:]:
        copy.wait_recv()

    strips = jnp.concatenate([window[REACH + i] for i in range(GROUP)], axis=1)
    plane_pairs = jnp.concatenate([pair_beta[i] for i in range(GROUP)], axis=1)
    density = lax.dot_general(
        strips, plane_pairs, (((1,), (1,)), ((), ())), preferred_element_type=F32
    )
    part[...] = density.astype(BF16).reshape(outer, share, pairs)
    part_copies = [
        remote(
            part.at[(z + d) % outer, pl.ds(c * sub, sub)],
            part_in.at[d - 1, pl.ds(c * sub, sub)],
            part_send.at[c, d - 1],
            part_recv.at[c, d - 1],
            plane(d),
        )
        for c in range(PIECES)
        for d in far_first
    ]

    near_copies[0].wait_recv()
    near_copies.append(
        remote(
            near.at[across], near.at[across], near_send.at[2], near_recv.at[2], core_mate
        )
    )
    own_rows.wait()
    pair_alpha[...] = jnp.transpose(pair_tile[...].astype(F32))
    own_coupling.wait()

    exc_copies = []
    for c in range(PIECES):
        piece = slice(c * sub, (c + 1) * sub)
        for copy in part_copies[c * (outer - 1) : (c + 1) * (outer - 1)]:
            copy.wait_recv()
        total = part[z, piece].astype(F32)
        for d in range(1, outer):
            total = total + part_in[d - 1, piece].astype(F32)
        raised = jnp.dot(total.astype(BF16), coupling[...], preferred_element_type=F32)
        at = pl.ds(pl.multiple_of(first % lanes + c * sub, sub), sub)
        excited[z, piece] = (raised * pair_alpha[at, :]).astype(BF16)
        exc_copies += [
            remote(
                excited.at[z, pl.ds(c * sub, sub)],
                excited.at[z, pl.ds(c * sub, sub)],
                exc_send.at[c, d - 1],
                exc_recv.at[c, d - 1],
                plane(d),
            )
            for d in far_first
        ]

    for copy in alpha_copies:
        copy.wait_recv()
    alpha_copy.wait()
    blocks = []
    for k in range(alpha_listed):
        off = (alpha_cols[0, k] - a + n_alpha) % n_alpha
        blocks.append(jnp.minimum(off, 1) + jnp.where(off > 1, 1, 0) if n_alpha > 2 else off)

    def alpha_step(i, carry):
        at = pl.ds(pl.multiple_of(i * strip, strip), strip)
        total = jnp.zeros((strip, width), F32)
        for k in range(alpha_listed):
            total = total + jnp.dot(
                alpha_ops[at, k * rows : (k + 1) * rows],
                coef[blocks[k]],
                preferred_element_type=F32,
            )
        out[at, :] = total
        return carry

    lax.fori_loop(0, GROUP, alpha_step, 0)

    for copy in near_copies[1:]:
        copy.wait_recv()
    for copy in halo_copies:
        copy.wait_recv()
    for i in range(GROUP):
        around = jnp.concatenate([window[i + s] for s in range(2 * REACH + 1)], axis=1)
        both[:, i * width : (i + 1) * width] = lax.dot_general(
            around, near[i], (((1,), (1,)), ((), ())), preferred_element_type=F32
        )

    back_copies = []
    for c in range(PIECES):
        piece = slice(c * sub, (c + 1) * sub)
        for e in sorted(range(outer), key=lambda d: min(d, outer - d)):
            if e > 0:
                exc_copies[c * (outer - 1) + far_first.index(e)].wait_recv()
            y = (z + outer - e) % outer
            mixed = jnp.dot(excited[y, piece], plane_pairs, preferred_element_type=F32)
            mixed = mixed + both[pl.ds(pl.multiple_of(y * share + c * sub, sub), sub), :]
            for i in range(GROUP):
                back[i, y, piece] = mixed[:, i * width : (i + 1) * width].astype(BF16)
            for i, h in enumerate((across, opposite, beside)):
                back_copies.append(
                    (
                        h,
                        y,
                        c,
                        i,
                        remote(
                            back.at[h, y, pl.ds(c * sub, sub)],
                            back_in.at[i, y, pl.ds(c * sub, sub)],
                            back_send.at[c * outer + e, i],
                            back_recv.at[c * outer + e, i],
                            (a, z * GROUP + h),
                        ),
                    )
                )
            at = pl.ds(pl.multiple_of(g * strip + y * share + c * sub, sub), sub)
            out[at, :] = out[at, :] + back[g, y, piece].astype(F32)
    for h, y, c, i, copy in back_copies:
        copy.wait_recv()
        at = pl.ds(pl.multiple_of(h * strip + y * share + c * sub, sub), sub)
        out[at, :] = out[at, :] + back_in[i, y, c * sub : (c + 1) * sub].astype(F32)

    everything = coef_copies + pair_copies + alpha_copies + near_copies + halo_copies
    everything += part_copies + exc_copies + [entry[-1] for entry in back_copies]
    for copy in everything:
        copy.wait_send()


def local(
    coef,
    beta_ops,
    beta_cols,
    alpha_ops,
    alpha_cols,
    pair_alpha,
    pair_beta,
    pair_coupling,
    denominators,
):
    n_alpha = lax.axis_size("alpha")
    n_beta = lax.axis_size("beta")
    rows, width = coef.shape
    pairs = pair_beta.shape[1]
    outer = n_beta // GROUP
    strip = rows // GROUP
    share = strip // outer
    lanes = max(width, share)
    span = 2 * REACH + 1
    dma = pltpu.SemaphoreType.DMA
    vmem, smem, anywhere = (
        pl.BlockSpec(memory_space=pltpu.VMEM),
        pl.BlockSpec(memory_space=pltpu.SMEM),
        pl.BlockSpec(memory_space=pl.ANY),
    )
    summed = pl.pallas_call(
        functools.partial(kernel, n_alpha, n_beta),
        out_shape=pltpu.VMEM((rows, width), F32),
        in_specs=[smem, smem] + [anywhere] * 6,
        out_specs=vmem,
        scratch_shapes=[
            pltpu.VMEM((min(n_alpha, 3), rows, width), BF16),
            pltpu.VMEM(beta_ops.shape, BF16),
            pltpu.VMEM(alpha_ops.shape, BF16),
            pltpu.VMEM((pairs, lanes), BF16),
            pltpu.VMEM((lanes, pairs), F32),
            pltpu.VMEM((GROUP, pairs, width), BF16),
            pltpu.VMEM((pairs, pairs), BF16),
            pltpu.VMEM((GROUP, width, span * width), BF16),
            pltpu.VMEM((GROUP + 2 * REACH, strip, width), BF16),
            pltpu.VMEM((outer, share, pairs), BF16),
            pltpu.VMEM((outer - 1, share, pairs), BF16),
            pltpu.VMEM((outer, share, pairs), BF16),
            pltpu.VMEM((strip, GROUP * width), F32),
            pltpu.VMEM((GROUP, outer, share, width), BF16),
            pltpu.VMEM((GROUP - 1, outer, share, width), BF16),
            dma((6,)),
            dma,
            dma((GROUP,)),
            dma((GROUP,)),
            dma((GROUP,)),
            dma((GROUP,)),
            dma((GROUP,)),
            dma((GROUP,)),
            dma((PIECES * outer, GROUP)),
            dma((PIECES * outer, GROUP)),
            dma((PIECES, outer - 1)),
            dma((PIECES, outer - 1)),
            dma((PIECES, outer - 1)),
            dma((PIECES, outer - 1)),
            dma((2,)),
            dma((2,)),
            dma((2,)),
            dma((2,)),
        ],
        compiler_params=pltpu.CompilerParams(collective_id=0, has_side_effects=True),
    )(beta_cols, alpha_cols, coef, beta_ops, alpha_ops, pair_alpha.T, pair_beta.T, pair_coupling)
    return summed / denominators


def solution(mesh):
    return jax.shard_map(
        local,
        mesh=mesh,
        in_specs=(
            P("alpha", "beta"),
            P("beta", None),
            P("beta", None),
            P("alpha", None),
            P("alpha", None),
            P("alpha", None),
            P("beta", None),
            P(),
            P("alpha", "beta"),
        ),
        out_specs=P("alpha", "beta"),
        check_vma=False,
    )
```
